32 devices in a mesh: ch: 4 (over z), sx: 4 (over x, core), sy: 2 (over y).
Axes of the slice: x: 2, y: 2, z: 4, core: 2. Of those that a mesh axis runs over, the one named last changes fastest.
Arguments:
- inputs: bfloat16 [768, 16, 4, 64], P('ch', 'sx', 'sy'), may hold values from -6 to 6
- pre_act: bfloat16 [768, 16, 4, 64], P('ch', 'sx', 'sy'), may hold values from -6 to 6
- out_grad: bfloat16 [768, 16, 4, 64], P('ch', 'sx', 'sy'), may hold values from -6 to 6
- weight_one: bfloat16 [27, 768, 768], P(None, 'ch'), may hold values from -0.0390625 to 0.0390625
- weight_two: bfloat16 [27, 768, 768], P(None, 'ch'), may hold values from -0.0390625 to 0.0390625
Outputs:
- input_grad: bfloat16 [768, 16, 4, 64], P('ch', 'sx', 'sy')
- filter_one_grad: float32 [27, 768, 768], P(None, 'ch')
- filter_two_grad: float32 [27, 768, 768], P(None, 'ch')
The draws below stay inside these ranges and needn't reach their ends.
All inputs are finite; a program needn't handle non-finite values.
Results may differ from the reference program's by a relative error of at most 0.0049.
Values may be sent and summed in bfloat16 or wider, within the bound.
A program may use at most 192 MiB of HBM per device.

```python
import math
import jax
import jax.numpy as jnp
from jax import lax

C = 768
NX = 16
NY = 4
NZ = 64


def block_levels(stream_key, extent, pieces, smallest, top_value):
    gain, own = 1.0, jax.random.fold_in(stream_key, 6)
    for dim, parts in pieces:
        steps = jnp.exp(jax.random.uniform(jax.random.fold_in(own, dim), (parts,), jnp.float32, smallest / len(pieces), top_value / len(pieces)))
        gain = gain * jnp.repeat(steps, extent[dim] // parts).reshape([-1 if axis == dim else 1 for axis in range(len(extent))])
    return gain


def scatter_about(own_key, extent, width, bound, shards=(), held_as=jnp.bfloat16):
    values = width * jax.random.normal(own_key, extent, jnp.float32)
    if shards:
        values = values * block_levels(own_key, extent, shards, -0.22, 0.18)
    return jnp.clip(values, -bound, bound).astype(held_as)


def setup_inputs(seed: int = 0) -> dict:
    seeds = jax.random.split(jax.random.key(seed), 6)
    return {
        "inputs": scatter_about(seeds[0], (C, NX, NY, NZ), 1.0, 6.0, ((0, 4), (1, 4), (2, 2))),
        "pre_act": scatter_about(seeds[1], (C, NX, NY, NZ), 1.0, 6.0, ((0, 4), (1, 4), (2, 2))),
        "out_grad": scatter_about(seeds[2], (C, NX, NY, NZ), 1.0, 6.0, ((0, 4), (1, 4), (2, 2))),
        "weight_one": scatter_about(seeds[3], (27, C, C), (27 * C) ** -0.5, 0.0390625, ((1, 4),)),
        "weight_two": scatter_about(seeds[4], (27, C, C), (27 * C) ** -0.5, 0.0390625, ((1, 4),)),
    }


def window(padded, offset, mirror):
    first = offset // 9
    second = offset // 3 % 3
    third = offset % 3
    if mirror:
        first, second, third = (2 - first, 2 - second, 2 - third)
    part = padded[:, first:first + NX, second:second + NY, third:third + NZ]
    return part.reshape(C, NX * NY * NZ)

def pad_all(array):
    return jnp.pad(array, ((0, 0), (1, 1), (1, 1), (1, 1)))

def contract_positions(left, right):
    return lax.dot_general(left, right, (((1,), (1,)), ((), ())), preferred_element_type=jnp.float32)

def reference(inputs, pre_act, out_grad, weight_one, weight_two):
    positions = NX * NY * NZ
    inputs_pad = pad_all(inputs)
    grad_pad = pad_all(out_grad)
    active_pad = pad_all(jnp.maximum(pre_act, jnp.zeros((), pre_act.dtype)))
    grad_flat = out_grad.reshape(C, positions)
    act_grad = jnp.zeros((C, positions), jnp.float32)
    filter_two = []
    for offset in range(27):
        act_grad = act_grad + jnp.dot(weight_two[offset], window(grad_pad, offset, True), preferred_element_type=jnp.float32)
        filter_two.append(contract_positions(window(active_pad, offset, False), grad_flat))
    delta = jnp.where(pre_act.reshape(C, positions) > 0, act_grad, 0.0).astype(jnp.bfloat16)
    delta_pad = pad_all(delta.reshape(C, NX, NY, NZ))
    input_grad = jnp.zeros((C, positions), jnp.float32)
    filter_one = []
    for offset in range(27):
        input_grad = input_grad + lax.dot_general(weight_one[offset], window(delta_pad, offset, True), (((0,), (0,)), ((), ())), preferred_element_type=jnp.float32)
        filter_one.append(contract_positions(delta, window(inputs_pad, offset, False)))
    factor = 1.0 / math.sqrt(positions)
    return (input_grad.reshape(C, NX, NY, NZ).astype(jnp.bfloat16), jnp.stack(filter_one) * factor, jnp.stack(filter_two) * factor)
```

```python
import math

import jax
import jax.numpy as jnp
from jax import lax
from jax.sharding import PartitionSpec as P


def padded_2(cells, sides, width):
    for axis, dim in sides:
        count = lax.axis_size(axis)
        ends = count - 1
        head = lax.slice_in_dim(cells, 0, width, axis=dim)
        tail = lax.slice_in_dim(cells, cells.shape[dim] - width, cells.shape[dim], axis=dim)
        cells = jnp.concatenate(
            [
                lax.ppermute(tail, axis, [(i, (i + 1) % count) for i in range(ends)]),
                cells,
                lax.ppermute(head, axis, [((i + 1) % count, i) for i in range(ends)]),
            ],
            axis=dim,
        )
    return cells


def window(padded, offset, mirror):
    first = offset // 9
    second = offset // 3 % 3
    third = offset % 3
    if mirror:
        first, second, third = (2 - first, 2 - second, 2 - third)
    size_x = padded.shape[1] - 2
    size_y = padded.shape[2] - 2
    size_z = padded.shape[3] - 2
    part = padded[:, first : first + size_x, second : second + size_y, third : third + size_z]
    return part.reshape(padded.shape[0], size_x * size_y * size_z)


def pad_depth(array):
    return jnp.pad(array, ((0, 0), (0, 0), (0, 0), (1, 1)))


def contract_positions(left, right):
    return lax.dot_general(
        left, right, (((1,), (1,)), ((), ())), preferred_element_type=jnp.float32
    )


def contract_first(left, right):
    return lax.dot_general(
        left, right, (((0,), (0,)), ((), ())), preferred_element_type=jnp.float32
    )


def spread_flat(array):
    padded = jnp.pad(array, ((0, 0), (0, 0), (0, 1), (0, 1)))
    return padded.reshape(padded.shape[0], -1)


def whole_window(blocks, counts):
    count_x, count_y = counts
    channels, size_x, size_y, size_z = blocks.shape[1:]
    grid = blocks.reshape(count_x, count_y, channels, size_x, size_y, size_z)
    grid = grid.transpose(2, 0, 3, 1, 4, 5)
    return grid.reshape(channels, count_x * size_x, count_y * size_y, size_z)


def column_slices(full, counts):
    ranks = counts[0] * counts[1]
    cut = full.reshape(ranks, full.shape[0] // ranks, *full.shape[1:])
    return whole_window(lax.all_to_all(cut, ("sx", "sy"), 0, 0, tiled=True), counts)


def shifts(size_y, size_z):
    row = size_z + 1
    plane = (size_y + 1) * row
    return [
        (a - 1) * plane + (b - 1) * row + c - 1
        for a in range(3)
        for b in range(3)
        for c in range(3)
    ]


def filter_slice(rows, columns, shift_rows):
    steps = shifts(rows.shape[2], rows.shape[3])
    margin = max(steps)
    left = spread_flat(rows)
    size = left.shape[1]
    right = jnp.pad(spread_flat(columns), ((0, 0), (margin, margin)))
    out = []
    for step in steps:
        start = margin - step if shift_rows else margin + step
        part = lax.slice_in_dim(right, start, start + size, axis=1)
        out.append(contract_positions(left, part))
    return jnp.stack(out)


def join_columns(part, factor):
    sent = (part * factor).astype(jnp.bfloat16)
    parts = lax.all_gather(sent, ("sx", "sy"), axis=0)
    return jnp.concatenate([parts[i] for i in range(parts.shape[0])], axis=2).astype(jnp.float32)


def shards(inputs, pre_act, out_grad, weight_one, weight_two):
    shape = pre_act.shape
    positions = shape[1] * shape[2] * shape[3]
    counts = (lax.axis_size("sx"), lax.axis_size("sy"))
    factor = 1.0 / math.sqrt(positions * counts[0] * counts[1])
    full_grad = lax.all_gather(out_grad, "ch", axis=0, tiled=True)
    active = jnp.maximum(pre_act, jnp.zeros((), pre_act.dtype))
    active_all = whole_window(lax.all_gather(active, ("sx", "sy"), axis=0), counts)
    grad_columns = column_slices(full_grad, counts)
    grad_pad = pad_depth(padded_2(full_grad, (("sx", 1), ("sy", 2)), 1))
    filter_two = join_columns(filter_slice(active_all, grad_columns, True), factor)
    act_grad = jnp.zeros((shape[0], positions), jnp.float32)
    for offset in range(27):
        act_grad = act_grad + jnp.dot(
            weight_two[offset], window(grad_pad, offset, True), preferred_element_type=jnp.float32
        )
    delta = jnp.where(pre_act.reshape(shape[0], positions) > 0, act_grad, 0.0).astype(jnp.bfloat16)
    delta = delta.reshape(shape)
    full_in = lax.all_gather(inputs, "ch", axis=0, tiled=True)
    input_columns = column_slices(full_in, counts)
    delta_all = whole_window(lax.all_gather(delta, ("sx", "sy"), axis=0), counts)
    filter_one = join_columns(filter_slice(delta_all, input_columns, False), factor)
    delta_pad = pad_depth(padded_2(delta, (("sx", 1), ("sy", 2)), 1))
    partial_terms = jnp.zeros((weight_one.shape[2], positions), jnp.float32)
    for offset in range(27):
        partial_terms = partial_terms + contract_first(
            weight_one[offset], window(delta_pad, offset, True)
        )
    partial_terms = partial_terms.reshape(weight_one.shape[2], shape[1], shape[2], shape[3])
    input_grad = lax.psum_scatter(partial_terms, "ch", scatter_dimension=0, tiled=True).astype(
        jnp.bfloat16
    )
    return (input_grad, filter_one, filter_two)


def solution(mesh):
    in_specs = (
        P("ch", "sx", "sy", None),
        P("ch", "sx", "sy", None),
        P("ch", "sx", "sy", None),
        P(None, "ch", None),
        P(None, "ch", None),
    )
    out_specs = (P("ch", "sx", "sy", None), P(None, "ch", None), P(None, "ch", None))
    return jax.shard_map(shards, mesh=mesh, in_specs=in_specs, out_specs=out_specs, check_vma=False)
```
